8 devices in a mesh: dp: 2 (over y, z), ep: 4 (over x, core).
Axes of the slice: x: 2, y: 2, z: 1, core: 2. Of those that a mesh axis runs over, the one named last changes fastest.
Arguments:
- x: bfloat16 [2, 4, 256, 7168], P('dp', 'ep'), parts along dimension 0
- expert: int32 [2, 4, 256, 8], P('dp', 'ep'), parts along dimension 0
- slot: int32 [2, 4, 256, 8], P('dp', 'ep'), parts along dimension 0
- gate: float32 [2, 4, 256, 8], P('dp', 'ep'), parts along dimension 0
- w_gate: bfloat16 [32, 7168, 2048], P('ep')
- w_up: bfloat16 [32, 7168, 2048], P('ep')
- w_down: bfloat16 [32, 2048, 7168], P('ep')
- s_gate: bfloat16 [7168, 2048], replicated
- s_up: bfloat16 [7168, 2048], replicated
- s_down: bfloat16 [2048, 7168], replicated
Outputs:
- y: bfloat16 [2, 4, 256, 7168], P('dp', 'ep'), parts along dimension 0
There are 2 independent parts. The reference program is written for one: setup_inputs(seed, part) draws one part's arguments, and reference() takes and returns one part's arrays. A program takes and returns all parts, laid end to end along the dimension named above; an argument that names none is the same for every part.
All inputs are finite; a program needn't handle non-finite values.
Results may differ from the reference program's by a relative error of at most 0.009.
Values are sent between devices in bfloat16 or wider.
A program may use at most 2 GiB of HBM per device.

```python
import jax
import jax.numpy as jnp

MEMBERS = 4
TOKENS = 256
D = 7168
FF = 2048
TOP = 8
EXPERTS = 32
SHARED_FF = 2048
SLOTS = 5 * TOKENS * TOP // (4 * EXPERTS)


def setup_inputs(seed: int = 0, part: int = 0) -> dict:
    own, k1, k2, k3, k4, k5, k6 = jax.random.split(jax.random.key(seed), 7)
    kx, ke, kl, kg = jax.random.split(jax.random.fold_in(own, part), 4)
    devices = (1, MEMBERS)
    place = jax.random.permutation(kl, jnp.arange(EXPERTS, dtype=jnp.uint32))
    slow = ((EXPERTS + (9 * place) % EXPERTS) << ((9 * place) // EXPERTS)) // EXPERTS
    wait = (jax.random.bits(ke, (*devices, TOKENS, EXPERTS), jnp.uint32) >> 10) * slow
    expert = jnp.argsort(wait, axis=-1)[..., :TOP].astype(jnp.int32)
    chosen = jax.nn.one_hot(expert, EXPERTS, dtype=jnp.int32)
    in_line = jnp.cumsum(chosen.reshape(*devices, TOKENS * TOP, EXPERTS), axis=2) - 1
    slot = jnp.sum(in_line.reshape(chosen.shape) * chosen, axis=-1)

    def one(key, rows, columns):
        return (jax.random.normal(key, (rows, columns), jnp.float32) * rows**-0.5).astype(jnp.bfloat16)

    def weights(key, rows, columns):
        return jax.lax.map(lambda k: one(k, rows, columns), jax.random.split(key, EXPERTS))

    return {
        "x": jax.random.normal(kx, (*devices, TOKENS, D), jnp.float32).astype(jnp.bfloat16),
        "expert": expert,
        "slot": slot,
        "gate": jax.nn.softmax(jax.random.normal(kg, expert.shape, jnp.float32)),
        "w_gate": weights(k1, D, FF),
        "w_up": weights(k2, D, FF),
        "w_down": weights(k3, FF, D),
        "s_gate": one(k4, D, SHARED_FF),
        "s_up": one(k5, D, SHARED_FF),
        "s_down": one(k6, SHARED_FF, D),
    }


def einsum(form, a, b):
    return jnp.einsum(form, a.astype(jnp.float32), b.astype(jnp.float32))


def for_all(x, s_gate, s_up, s_down):
    h = jax.nn.silu(einsum("...d,df->...f", x, s_gate)) * einsum("...d,df->...f", x, s_up)
    return einsum("...f,fd->...d", h.astype(jnp.bfloat16), s_down)


def reference(x, expert, slot, gate, w_gate, w_up, w_down, s_gate, s_up, s_down):
    to_expert = jax.nn.one_hot(expert, EXPERTS, dtype=jnp.bfloat16)
    to_slot = jax.nn.one_hot(slot, SLOTS, dtype=jnp.bfloat16)
    weighted = to_expert * gate[..., None].astype(jnp.bfloat16)
    dispatch = einsum("abtke,abtkc->abtec", to_expert, to_slot).astype(jnp.bfloat16)
    combine = einsum("abtke,abtkc->abtec", weighted, to_slot).astype(jnp.bfloat16)
    z = einsum("abtec,abtd->aebcd", dispatch, x).astype(jnp.bfloat16)
    h = jax.nn.silu(einsum("aebcd,edf->aebcf", z, w_gate))
    h = (h * einsum("aebcd,edf->aebcf", z, w_up)).astype(jnp.bfloat16)
    out = einsum("aebcf,efd->aebcd", h, w_down).astype(jnp.bfloat16)
    y = einsum("abtec,aebcd->abtd", combine, out)
    return (y + for_all(x, s_gate, s_up, s_down)).astype(jnp.bfloat16)
```

```python
import functools

import jax
import jax.numpy as jnp
from jax import lax
from jax.experimental import pallas as pl
from jax.experimental.pallas import tpu as pltpu
from jax.sharding import PartitionSpec as P

HALF = 160
SEG = 80
MESH = pl.DeviceIdType.MESH
F32, BF16 = jnp.float32, jnp.bfloat16
ANY = pl.BlockSpec(memory_space=pl.ANY)
VMEM = pl.BlockSpec(memory_space=pltpu.VMEM)
SMEM = pl.BlockSpec(memory_space=pltpu.SMEM)


def offsets(npad, e):
    offs, total = [], 0
    for k in range(4):
        offs.append(total)
        total = total + npad[k, e]
    return offs, total


def up_kernel(tile, depth, npad, st, x0, x1, x2, x3, wg, wu, h, xv, z, wbuf, hbuf, hout, xsem, wsem, hsem):
    experts, rows, ff = wg.shape
    per = ff // tile
    steps = experts * per

    def weights(i):
        e, cols, s = i // per, pl.ds(pl.multiple_of((i % per) * tile, tile), tile), i % depth
        return [
            pltpu.make_async_copy(w.at[e, :, cols], wbuf.at[s, :, pl.ds(n * tile, tile)], wsem.at[s, n])
            for n, w in enumerate((wg, wu))
        ]

    def result(e):
        return pltpu.make_async_copy(hout.at[e % 2], h.at[e], hsem.at[e % 2])

    blocks = [pltpu.make_async_copy(x, xv.at[k], xsem.at[k]) for k, x in enumerate((x0, x1, x2, x3))]
    for c in blocks:
        c.start()
    for i in range(depth):
        for c in weights(i):
            c.start()
    for c in blocks:
        c.wait()

    def dispatch(e):
        offs, _ = offsets(npad, e)
        line = lax.broadcasted_iota(jnp.int32, (SEG, xv.shape[1]), 0)
        for k in range(4):
            pick = jnp.where(line == st[k, e], 1.0, 0.0).astype(BF16)
            at = pl.ds(pl.multiple_of(offs[k], 16), SEG)
            z[at, :] = jnp.dot(pick, xv[k], preferred_element_type=F32).astype(BF16)

    def step(i, _):
        e, j, s = i // per, i % per, i % depth
        offs, total = offsets(npad, e)

        @pl.when(j == 0)
        def _():
            dispatch(e)

        for c in weights(i):
            c.wait()

        def work(n):
            gu = jnp.dot(z[:n, :], wbuf[s], preferred_element_type=F32)
            g, u = gu[:, :tile], gu[:, tile:]
            hbuf[:n, pl.ds(pl.multiple_of(j * tile, tile), tile)] = (jax.nn.silu(g) * u).astype(BF16)

        @pl.when((total > 0) & (total <= HALF))
        def _():
            work(HALF)

        @pl.when(total > HALF)
        def _():
            work(2 * HALF)

        @pl.when(i + depth < steps)
        def _():
            for c in weights(i + depth):
                c.start()

        @pl.when(j == per - 1)
        def _():
            @pl.when(e >= 2)
            def _():
                result(e).wait()

            line = lax.broadcasted_iota(jnp.int32, (SEG, ff), 0)
            for k in range(4):
                part = hbuf[pl.ds(pl.multiple_of(offs[k], 16), SEG), :]
                hout[e % 2, SEG * k : SEG * (k + 1), :] = jnp.where(line < npad[k, e], part, jnp.zeros_like(part))
            result(e).start()

        return 0

    lax.fori_loop(0, steps, step, 0)
    for e in (experts - 2, experts - 1):
        result(e).wait()


def up_call(npad, st, xs, wg, wu):
    experts, rows, ff = wg.shape
    tile, depth = 256, 4
    tokens = xs[0].shape[0]
    return pl.pallas_call(
        functools.partial(up_kernel, tile, depth),
        out_shape=jax.ShapeDtypeStruct((experts, 2 * HALF, ff), BF16),
        in_specs=[SMEM, VMEM] + [ANY] * 6,
        out_specs=ANY,
        scratch_shapes=[
            pltpu.VMEM((4, tokens, rows), BF16),
            pltpu.VMEM((2 * HALF, rows), BF16),
            pltpu.VMEM((depth, rows, 2 * tile), BF16),
            pltpu.VMEM((2 * HALF, ff), BF16),
            pltpu.VMEM((2, 2 * HALF, ff), BF16),
            pltpu.SemaphoreType.DMA((4,)),
            pltpu.SemaphoreType.DMA((depth, 2)),
            pltpu.SemaphoreType.DMA((2,)),
        ],
        compiler_params=pltpu.CompilerParams(vmem_limit_bytes=60 * 2**20),
        cost_estimate=pl.CostEstimate(
            flops=2 * experts * HALF * rows * ff * 2, bytes_accessed=experts * rows * ff * 4, transcendentals=0
        ),
        name="up",
    )(npad, st, *xs, wg, wu)


def down_kernel(tiles, tile, depth, sc, gc, h, wd, shared, y, hv, wbuf, rows, mix, own, far32, outs, lands, sbuf, ybuf, hsem, wsem, ssem, ysem, send, recv):
    experts, ff, _ = wd.shape
    steps = tiles * experts
    tokens, room = mix.shape[1:]
    me = lax.axis_index("ep")
    near, far = me + 1 - 2 * (me % 2), (me + 2) % 4

    barrier = pltpu.get_barrier_semaphore()
    for d in (near, far):
        pl.semaphore_signal(barrier, inc=1, device_id={"ep": d}, device_id_type=MESH)

    def columns(t):
        return pl.ds(pl.multiple_of(t * tile, tile), tile)

    def weights(i):
        s = i % depth
        return pltpu.make_async_copy(wd.at[i % experts, :, columns(i // experts)], wbuf.at[s], wsem.at[s])

    def addend(t):
        return pltpu.make_async_copy(shared.at[:, columns(t)], sbuf.at[t % 2], ssem.at[t % 2])

    def result(t):
        return pltpu.make_async_copy(ybuf.at[t % 2], y.at[:, columns(t)], ysem.at[t % 2])

    def sending(kind, t):
        return pltpu.make_async_remote_copy(
            src_ref=outs.at[kind, t % 2],
            dst_ref=lands.at[kind, t],
            send_sem=send.at[kind, t],
            recv_sem=recv.at[kind, t],
            device_id={"ep": far if kind == 2 else near},
            device_id_type=MESH,
        )

    loads = [pltpu.make_async_copy(h.at[e], hv.at[e], hsem.at[e]) for e in range(experts)]
    loads[0].start()
    weights(0).start()
    for c in loads[1:]:
        c.start()
    for i in range(1, depth):
        weights(i).start()
    for t in range(2):
        addend(t).start()
    place = lax.broadcasted_iota(jnp.int32, (tokens, room), 1)
    for k in range(4):
        m = jnp.zeros((tokens, room), F32)
        for e in range(experts):
            s = sc[k, :, e : e + 1]
            s = jnp.where(s >= 0, s + SEG * e, -1)
            m = jnp.where(place == s, gc[k, :, e : e + 1], m)
        mix[k] = m.astype(BF16)
    pl.semaphore_wait(barrier, 2)
    for c in loads:
        c.wait()

    def combine(t):
        @pl.when(t >= 2)
        def _():
            sending(0, t - 2).wait_send()
            sending(1, t - 2).wait_send()

        outs[0, t % 2] = jnp.dot(mix[1], rows[1], preferred_element_type=F32).astype(BF16)
        outs[1, t % 2] = jnp.dot(mix[3], rows[3], preferred_element_type=F32).astype(BF16)
        far32[t % 2] = jnp.dot(mix[2], rows[2], preferred_element_type=F32)
        own[t % 4] = jnp.dot(mix[0], rows[0], preferred_element_type=F32)
        sending(1, t).start()
        sending(0, t).start()

    def forward(t):
        sending(1, t).wait_recv()

        @pl.when(t >= 2)
        def _():
            sending(2, t - 2).wait_send()

        outs[2, t % 2] = (far32[t % 2] + lands[1, t].astype(F32)).astype(BF16)
        sending(2, t).start()

    def final(t):
        sending(0, t).wait_recv()
        sending(2, t).wait_recv()
        addend(t).wait()

        @pl.when(t >= 2)
        def _():
            result(t - 2).wait()

        ybuf[t % 2] = (own[t % 4] + sbuf[t % 2] + lands[0, t].astype(F32) + lands[2, t].astype(F32)).astype(BF16)
        result(t).start()

        @pl.when(t + 2 < tiles)
        def _():
            addend(t + 2).start()

    def step(i, _):
        t, e, s = i // experts, i % experts, i % depth
        weights(i).wait()
        o = jnp.dot(hv[e], wbuf[s], preferred_element_type=F32).astype(BF16)
        for k in range(4):
            rows[k, pl.ds(pl.multiple_of(e * SEG, 16), SEG), :] = o[SEG * k : SEG * (k + 1)]

        @pl.when(i + depth < steps)
        def _():
            weights(i + depth).start()

        @pl.when((e == 1) & (t >= 1))
        def _():
            forward(t - 1)

        @pl.when((e == 5) & (t >= 2))
        def _():
            final(t - 2)

        @pl.when(e == experts - 1)
        def _():
            combine(t)

        return 0

    lax.fori_loop(0, steps, step, 0)
    last = jnp.int32(tiles - 1)
    forward(last)
    final(last - 1)
    final(last)
    for t in (tiles - 2, tiles - 1):
        result(t).wait()
        for kind in range(3):
            sending(kind, t).wait_send()


def down_call(sc, gc, h, wd, shared):
    experts, ff, width = wd.shape
    tile, depth = 1024, 3
    tiles = width // tile
    tokens = sc.shape[1]
    room = SEG * experts
    return pl.pallas_call(
        functools.partial(down_kernel, tiles, tile, depth),
        out_shape=jax.ShapeDtypeStruct((tokens, width), BF16),
        in_specs=[VMEM, VMEM, ANY, ANY, ANY],
        out_specs=ANY,
        scratch_shapes=[
            pltpu.VMEM((experts, 4 * SEG, ff), BF16),
            pltpu.VMEM((depth, ff, tile), BF16),
            pltpu.VMEM((4, room, tile), BF16),
            pltpu.VMEM((4, tokens, room), BF16),
            pltpu.VMEM((4, tokens, tile), F32),
            pltpu.VMEM((2, tokens, tile), F32),
            pltpu.VMEM((3, 2, tokens, tile), BF16),
            pltpu.VMEM((3, tiles, tokens, tile), BF16),
            pltpu.VMEM((2, tokens, tile), F32),
            pltpu.VMEM((2, tokens, tile), BF16),
            pltpu.SemaphoreType.DMA((experts,)),
            pltpu.SemaphoreType.DMA((depth,)),
            pltpu.SemaphoreType.DMA((2,)),
            pltpu.SemaphoreType.DMA((2,)),
            pltpu.SemaphoreType.DMA((3, tiles)),
            pltpu.SemaphoreType.DMA((3, tiles)),
        ],
        compiler_params=pltpu.CompilerParams(vmem_limit_bytes=63 * 2**20, collective_id=0, has_side_effects=True),
        cost_estimate=pl.CostEstimate(
            flops=2 * experts * 4 * SEG * width * ff, bytes_accessed=experts * width * ff * 2, transcendentals=0
        ),
        name="down",
    )(sc, gc, h, wd, shared)


def solution(mesh):
    members = mesh.shape["ep"]

    def move(v, hop):
        return lax.ppermute(v, "ep", [(i, i ^ hop) for i in range(members)])

    def body(x, expert, slot, gate, wg, wu, wd, sg, su, sd):
        x, expert, slot, gate = (v[0, 0] for v in (x, expert, slot, gate))
        local = wg.shape[0]
        me = lax.axis_index("ep")
        far_x = move(x, 2)
        near_x = move(x, 1)

        hit = (expert[:, :, None] == jnp.arange(local * members)) & (slot < SEG)[:, :, None]
        slots = jnp.max(jnp.where(hit, slot[:, :, None], -1), axis=1)
        gates = jnp.sum(jnp.where(hit, gate.astype(BF16).astype(F32)[:, :, None], 0.0), axis=1)
        table = jnp.stack([slots.astype(F32), gates])
        parts = []
        for hop in range(members):
            part = lax.dynamic_slice_in_dim(table, (me ^ hop) * local, local, axis=2)
            parts.append(move(part, hop) if hop else part)
        table = jnp.stack(parts)
        sc, gc = table[:, 0].astype(jnp.int32), table[:, 1]
        npad = (jnp.max(sc, axis=1) + 16) // 16 * 16
        st = jnp.swapaxes(sc, 1, 2)[:, :, None, :]

        g = jnp.dot(x, sg, preferred_element_type=F32)
        u = jnp.dot(x, su, preferred_element_type=F32)
        shared = jnp.dot((jax.nn.silu(g) * u).astype(BF16), sd, preferred_element_type=F32)

        shared, far_x = lax.optimization_barrier((shared, far_x))
        diag_x = move(far_x, 1)
        h = up_call(npad, st, (x, near_x, far_x, diag_x), wg, wu)

        return down_call(sc, gc, h, wd, shared)[None, None]

    tok, exp, whole = P("dp", "ep", None, None), P("ep", None, None), P(None, None)
    return jax.shard_map(
        body,
        mesh=mesh,
        in_specs=(tok, tok, tok, tok, exp, exp, exp, whole, whole, whole),
        out_specs=tok,
        check_vma=False,
    )
```

```python
import functools

import jax
import jax.numpy as jnp
from jax import lax
from jax.experimental import pallas as pl
from jax.experimental.pallas import tpu as pltpu
from jax.sharding import PartitionSpec as P


FIRST = 2304
UNIT = 256
HALF = 160
SEG = 80
MESH = pl.DeviceIdType.MESH
F32, BF16 = jnp.float32, jnp.bfloat16
ANY = pl.BlockSpec(memory_space=pl.ANY)
VMEM = pl.BlockSpec(memory_space=pltpu.VMEM)
SMEM = pl.BlockSpec(memory_space=pltpu.SMEM)


def offsets(npad, e):
    offs, total = [], 0
    for k in range(4):
        offs.append(total)
        total = total + npad[k, e]
    return offs, total


def up_kernel(first, tile, depth, npad, table, x0, x1, x2, x3, wg, wu, *refs):
    (sums, h, xv, z, wbuf, abuf, hbuf, hout, xsem, wsem, asem, hsem), begins = refs, first == 0
    experts, ff, rows = wg.shape[0], wg.shape[2], z.shape[1]
    per = ff // tile
    steps = experts * per
    units = tile // UNIT
    ring = abuf.shape[0]

    def weights(i):
        e, cols, s = i // per, pl.ds(pl.multiple_of((i % per) * tile, tile), tile), i % depth
        return [
            pltpu.make_async_copy(
                w.at[e, pl.ds(first, rows), cols], wbuf.at[s, :, pl.ds(n * tile, tile)], wsem.at[s, n]
            )
            for n, w in enumerate((wg, wu))
        ]

    def partial(i, act):
        e, j, s = i // per, i % per, i % ring
        _, total = offsets(npad, e)
        for b in range(4):
            band = pl.ds(b * SEG, SEG)
            near, away = abuf.at[s, :, band], sums.at[e, pl.ds(j * units, units), band]

            @pl.when(total > b * SEG)
            def _():
                act(pltpu.make_async_copy(*((near, away) if begins else (away, near)), asem.at[s, b]))

    def result(e):
        return pltpu.make_async_copy(hout.at[e % 2], h.at[e], hsem.at[e % 2])

    def ask(i):
        for c in weights(i):
            c.start()
        if not begins:
            partial(i, lambda c: c.start())

    blocks = []
    for k, x in enumerate((x0, x1, x2, x3)):
        part = x if x.shape[1] == rows else x.at[:, pl.ds(first, rows)]
        blocks.append(pltpu.make_async_copy(part, xv.at[k], xsem.at[k]))
    for c in blocks:
        c.start()
    for i in range(depth):
        ask(i)
    for c in blocks:
        c.wait()

    def dispatch(e):
        offs, _ = offsets(npad, e)
        line = lax.broadcasted_iota(jnp.int32, (SEG, xv.shape[1]), 0).astype(F32)
        for k in range(4):
            pick = jnp.where(line == table[k, 0, pl.ds(e, 1), :], 1.0, 0.0).astype(BF16)
            at = pl.ds(pl.multiple_of(offs[k], 16), SEG)
            z[at, :] = jnp.dot(pick, xv[k], preferred_element_type=F32).astype(BF16)

    def step(i, _):
        e, j, s, a = i // per, i % per, i % depth, i % ring
        offs, total = offsets(npad, e)

        @pl.when(j == 0)
        def _():
            dispatch(e)

        for c in weights(i):
            c.wait()
        if begins:

            @pl.when(i >= ring)
            def _():
                partial(i - ring, lambda c: c.wait())
        else:
            partial(i, lambda c: c.wait())

        def work(n):
            gu = jnp.dot(z[:n, :], wbuf[s], preferred_element_type=F32)
            for v in range(units):
                g, u = (gu[:, m * tile + v * UNIT :][:, :UNIT] for m in range(2))
                if begins:
                    abuf[a, v, :n, :UNIT] = g
                    abuf[a, v, :n, UNIT:] = u
                else:
                    g, u = g + abuf[a, v, :n, :UNIT], u + abuf[a, v, :n, UNIT:]
                    cols = pl.ds(pl.multiple_of(j * tile + v * UNIT, UNIT), UNIT)
                    hbuf[:n, cols] = (jax.nn.silu(g) * u).astype(BF16)

        @pl.when((total > 0) & (total <= HALF))
        def _():
            work(HALF)

        @pl.when(total > HALF)
        def _():
            work(2 * HALF)

        @pl.when(i + depth < steps)
        def _():
            ask(i + depth)

        if begins:
            partial(i, lambda c: c.start())
            return 0

        @pl.when(j == per - 1)
        def _():
            @pl.when(e >= 2)
            def _():
                result(e).wait()

            line = lax.broadcasted_iota(jnp.int32, (SEG, ff), 0)
            for k in range(4):
                part = hbuf[pl.ds(pl.multiple_of(offs[k], 16), SEG), :]
                hout[e % 2, SEG * k : SEG * (k + 1), :] = jnp.where(line < npad[k, e], part, jnp.zeros_like(part))
            result(e).start()

        return 0

    lax.fori_loop(0, steps, step, 0)
    if begins:
        for i in range(steps - ring, steps):
            partial(jnp.int32(i), lambda c: c.wait())
    else:
        for e in (experts - 2, experts - 1):
            result(e).wait()


def begin_kernel(tile, depth, npad, table, x0, x1, x2, x3, wg, wu, sums, xv, z, wbuf, abuf, xsem, wsem, asem):
    refs = (sums, None, xv, z, wbuf, abuf, None, None, xsem, wsem, asem, None)
    up_kernel(0, tile, depth, npad, table, x0, x1, x2, x3, wg, wu, *refs)


def up_call(first, rows, npad, table, xs, wg, wu, sums=None):
    experts, _, ff = wg.shape
    tile, depth = (512, 4) if first == 0 else (512, 3)
    ring, units = (2 if first == 0 else depth), tile // UNIT
    tokens = xs[0].shape[0]
    scratch = [
        pltpu.VMEM((4, tokens, rows), BF16),
        pltpu.VMEM((2 * HALF, rows), BF16),
        pltpu.VMEM((depth, rows, 2 * tile), BF16),
        pltpu.VMEM((ring, units, 2 * HALF, 2 * UNIT), F32),
    ]
    semaphores = [
        pltpu.SemaphoreType.DMA((4,)),
        pltpu.SemaphoreType.DMA((depth, 2)),
        pltpu.SemaphoreType.DMA((ring, 4)),
    ]
    common = dict(
        compiler_params=pltpu.CompilerParams(vmem_limit_bytes=63 * 2**20),
        cost_estimate=pl.CostEstimate(
            flops=2 * experts * HALF * rows * ff * 2, bytes_accessed=experts * rows * ff * 4, transcendentals=0
        ),
    )
    if first == 0:
        return pl.pallas_call(
            functools.partial(begin_kernel, tile, depth),
            out_shape=jax.ShapeDtypeStruct((experts, ff // UNIT, 2 * HALF, 2 * UNIT), F32),
            in_specs=[SMEM, VMEM] + [ANY] * 6,
            out_specs=ANY,
            scratch_shapes=scratch + semaphores,
            name="up_first",
            **common,
        )(npad, table, *xs, wg, wu)
    return pl.pallas_call(
        functools.partial(up_kernel, first, tile, depth),
        out_shape=jax.ShapeDtypeStruct((experts, 2 * HALF, ff), BF16),
        in_specs=[SMEM, VMEM] + [ANY] * 7,
        out_specs=ANY,
        scratch_shapes=scratch
        + [pltpu.VMEM((2 * HALF, ff), BF16), pltpu.VMEM((2, 2 * HALF, ff), BF16)]
        + semaphores
        + [pltpu.SemaphoreType.DMA((2,))],
        name="up_rest",
        **common,
    )(npad, table, *xs, wg, wu, sums)


def shared_kernel(tile, wide, depth, x, sg, su, sd, y, rest, xv, wbuf, dbuf, hbuf, ybuf, xsem, wsem, dsem, ysem):
    ff, width = sd.shape
    ups, downs = ff // tile, width // wide

    def block(n, size):
        return pl.ds(pl.multiple_of(n * size, size), size)

    def up(i):
        return [
            pltpu.make_async_copy(
                w.at[:, block(i, tile)], wbuf.at[i % depth, :, pl.ds(n * tile, tile)], wsem.at[i % depth, n]
            )
            for n, w in enumerate((sg, su))
        ]

    def down(t):
        return pltpu.make_async_copy(sd.at[:, block(t, wide)], dbuf.at[t % depth], dsem.at[t % depth])

    def result(t):
        return pltpu.make_async_copy(ybuf.at[t % 2], y.at[:, block(t, wide)], ysem.at[t % 2])

    load = pltpu.make_async_copy(x, xv, xsem)
    load.start()
    for i in range(depth):
        for c in up(i):
            c.start()
    load.wait()
    split = pltpu.make_async_copy(xv.at[:, x.shape[1] - rest.shape[1] :], rest, xsem)
    split.start()

    def raise_(i, _):
        for c in up(i):
            c.wait()
        gu = jnp.dot(xv[...], wbuf[i % depth], preferred_element_type=F32)
        hbuf[:, block(i, tile)] = (jax.nn.silu(gu[:, :tile]) * gu[:, tile:]).astype(BF16)

        @pl.when(i + depth < ups)
        def _():
            for c in up(i + depth):
                c.start()

        @pl.when(i >= ups - depth)
        def _():
            down(i - (ups - depth)).start()

        return 0

    lax.fori_loop(0, ups, raise_, 0)

    def lower(t, _):
        down(t).wait()

        @pl.when(t >= 2)
        def _():
            result(t - 2).wait()

        ybuf[t % 2] = jnp.dot(hbuf[...], dbuf[t % depth], preferred_element_type=F32)
        result(t).start()

        @pl.when(t + depth < downs)
        def _():
            down(t + depth).start()

        return 0

    lax.fori_loop(0, downs, lower, 0)
    for t in (downs - 2, downs - 1):
        result(t).wait()
    split.wait()


def shared_call(x, sg, su, sd):
    tokens, rows = x.shape
    ff, width = sd.shape
    tile, wide, depth = 256, 1024, 4
    return pl.pallas_call(
        functools.partial(shared_kernel, tile, wide, depth),
        out_shape=[
            jax.ShapeDtypeStruct((tokens, width), F32),
            jax.ShapeDtypeStruct((tokens, rows - FIRST), BF16),
        ],
        in_specs=[ANY] * 4,
        out_specs=[ANY] * 2,
        scratch_shapes=[
            pltpu.VMEM((tokens, rows), BF16),
            pltpu.VMEM((depth, rows, 2 * tile), BF16),
            pltpu.VMEM((depth, ff, wide), BF16),
            pltpu.VMEM((tokens, ff), BF16),
            pltpu.VMEM((2, tokens, wide), F32),
            pltpu.SemaphoreType.DMA,
            pltpu.SemaphoreType.DMA((depth, 2)),
            pltpu.SemaphoreType.DMA((depth,)),
            pltpu.SemaphoreType.DMA((2,)),
        ],
        compiler_params=pltpu.CompilerParams(vmem_limit_bytes=63 * 2**20),
        cost_estimate=pl.CostEstimate(
            flops=6 * tokens * rows * ff, bytes_accessed=6 * rows * ff, transcendentals=0
        ),
        name="shared",
    )(x, sg, su, sd)


def down_kernel(tile, small, table, h, wd, shared, y, hv, wbuf, rows, mix, own, far32, outs, lands, sbuf, ybuf, hsem, wsem, ssem, ysem, send, recv):
    experts, _, width = wd.shape
    _, room = mix.shape[1:]
    pairs = experts // 2
    many = width // tile - 1
    few = tile // small
    me = lax.axis_index("ep")
    near, far = me + 1 - 2 * (me % 2), (me + 2) % 4

    barrier = pltpu.get_barrier_semaphore()
    for d in (near, far):
        pl.semaphore_signal(barrier, inc=1, device_id={"ep": d}, device_id_type=MESH)

    class Tile:
        def __init__(self, t, part=None):
            self.t = t if part is None else many + part
            self.n = tile if part is None else small
            start = t * tile if part is None else many * tile + part * small
            self.columns = pl.ds(pl.multiple_of(start, small), self.n)
            self.place = t if part is None else many
            self.inside = pl.ds(0 if part is None else part * small, self.n)

        def addend(self):
            s = self.t % 2
            return pltpu.make_async_copy(shared.at[:, self.columns], sbuf.at[s, :, : self.n], ssem.at[s])

        def result(self):
            s = self.t % 2
            return pltpu.make_async_copy(ybuf.at[s, :, : self.n], y.at[:, self.columns], ysem.at[s])

        def sending(self, kind):
            return pltpu.make_async_remote_copy(
                src_ref=outs.at[kind, self.t % 2, :, : self.n],
                dst_ref=lands.at[kind, self.place, :, self.inside],
                send_sem=send.at[kind, self.t],
                recv_sem=recv.at[kind, self.t],
                device_id={"ep": far if kind == 2 else near},
                device_id_type=MESH,
            )

        def combine(self, older):
            n, s = self.n, self.t % 2

            def free(old):
                old.sending(0).wait_send()
                old.sending(1).wait_send()

            older(free)
            outs[0, s, :, :n] = jnp.dot(mix[1], rows[1, :, :n], preferred_element_type=F32).astype(BF16)
            outs[1, s, :, :n] = jnp.dot(mix[3], rows[3, :, :n], preferred_element_type=F32).astype(BF16)
            far32[s, :, :n] = jnp.dot(mix[2], rows[2, :, :n], preferred_element_type=F32)
            own[self.t % 4, :, :n] = jnp.dot(mix[0], rows[0, :, :n], preferred_element_type=F32)
            self.sending(1).start()
            self.sending(0).start()

        def forward(self, older):
            n, s = self.n, self.t % 2
            self.sending(1).wait_recv()
            older(lambda old: old.sending(2).wait_send())
            outs[2, s, :, :n] = (far32[s, :, :n] + lands[1, self.place, :, self.inside].astype(F32)).astype(BF16)
            self.sending(2).start()

        def final(self, older, newer):
            n, s = self.n, self.t % 2
            self.sending(0).wait_recv()
            self.sending(2).wait_recv()
            self.addend().wait()
            older(lambda old: old.result().wait())
            local = own[self.t % 4, :, :n] + sbuf[s, :, :n]
            rest = (lands[k, self.place, :, self.inside].astype(F32) for k in (0, 2))
            ybuf[s, :, :n] = (local + next(rest) + next(rest)).astype(BF16)
            self.result().start()
            newer(lambda new: new.addend().start())

    def weights(t, p):
        q = (t.t * pairs + p) % 2
        return [
            pltpu.make_async_copy(
                wd.at[2 * p + m, :, t.columns], wbuf.at[2 * q + m, :, : t.n], wsem.at[2 * q + m]
            )
            for m in range(2)
        ]

    def start(copies):
        for c in copies:
            c.start()

    def load(e):
        return pltpu.make_async_copy(h.at[e], hv.at[e], hsem.at[e])

    def multiply(t, p):
        q = (t.t * pairs + p) % 2
        for c in weights(t, p):
            c.wait()
        for m in range(2):
            e = 2 * p + m
            o = jnp.dot(hv[e], wbuf[2 * q + m, :, : t.n], preferred_element_type=F32).astype(BF16)
            for k in range(4):
                rows[k, pl.ds(pl.multiple_of(e * SEG, 16), SEG), : t.n] = o[SEG * k : SEG * (k + 1)]

    for p in range(2):
        load(2 * p).start()
        load(2 * p + 1).start()
        start(weights(Tile(0), p))
    for e in range(4, experts):
        load(e).start()
    for t in range(2):
        Tile(t).addend().start()

    place, row = (lax.broadcasted_iota(jnp.int32, (experts, room), d) for d in (1, 0))
    spread = jnp.where((place >= SEG * row) & (place < SEG * (row + 1)), 1.0, 0.0).astype(BF16)
    place = lax.broadcasted_iota(jnp.int32, (1, room), 1)
    slot = place
    for e in range(1, experts):
        slot = jnp.where(place >= SEG * e, place - SEG * e, slot)
    slot = slot.astype(F32)
    for k in range(4):
        s, g = (
            lax.dot_general(table[k, n].astype(BF16), spread, (((0,), (0,)), ((), ())), preferred_element_type=F32)
            for n in range(2)
        )
        mix[k] = jnp.where(s == slot, g, 0.0).astype(BF16)
    pl.semaphore_wait(barrier, 2)

    def step(i, _):
        t, p = i // pairs, i % pairs
        this = Tile(t)

        def back(least, distance):
            def older(act):
                @pl.when(t >= least)
                def _():
                    act(Tile(t - distance))

            return older

        @pl.when(t == 0)
        def _():
            load(2 * p).wait()
            load(2 * p + 1).wait()

        multiply(this, p)

        @pl.when(i + 2 < many * pairs)
        def _():
            start(weights(Tile((i + 2) // pairs), (i + 2) % pairs))

        @pl.when(i + 2 >= many * pairs)
        def _():
            start(weights(Tile(0, 0), i + 2 - many * pairs))

        @pl.when((p == 0) & (t >= 1))
        def _():
            Tile(t - 1).forward(back(3, 3))

        @pl.when((p == 2) & (t >= 2))
        def _():
            Tile(t - 2).final(back(4, 4), lambda act: act(Tile(t)))

        @pl.when(p == pairs - 1)
        def _():
            this.combine(back(2, 2))

        return 0

    lax.fori_loop(0, many * pairs, step, 0)

    tiles = [Tile(t) for t in range(many)] + [Tile(0, m) for m in range(few)]

    def at(n):
        return lambda act: act(tiles[n])

    for n in range(many, many + few):

        def step2(p, _):
            multiply(tiles[n], p)

            @pl.when(p + 2 < pairs)
            def _():
                start(weights(tiles[n], p + 2))

            if n + 1 < many + few:

                @pl.when(p + 2 >= pairs)
                def _():
                    start(weights(tiles[n + 1], p + 2 - pairs))

            @pl.when(p == 0)
            def _():
                tiles[n - 1].forward(at(n - 3))

            @pl.when(p == 2)
            def _():
                tiles[n - 2].final(at(n - 4), at(n))

            return 0

        lax.fori_loop(0, pairs, step2, 0)
        tiles[n].combine(at(n - 2))
    last = many + few - 1
    tiles[last].forward(at(last - 2))
    tiles[last - 1].final(at(last - 3), lambda act: None)
    tiles[last].final(at(last - 2), lambda act: None)
    for t in tiles[-2:]:
        t.result().wait()
        for kind in range(3):
            t.sending(kind).wait_send()


def down_call(table, h, wd, shared):
    experts, ff, width = wd.shape
    tile, small = 1024, 512
    tiles = width // tile
    count = tiles - 1 + tile // small
    tokens = table.shape[3]
    room = SEG * experts
    return pl.pallas_call(
        functools.partial(down_kernel, tile, small),
        out_shape=jax.ShapeDtypeStruct((tokens, width), BF16),
        in_specs=[VMEM, ANY, ANY, ANY],
        out_specs=ANY,
        scratch_shapes=[
            pltpu.VMEM((experts, 4 * SEG, ff), BF16),
            pltpu.VMEM((4, ff, tile), BF16),
            pltpu.VMEM((4, room, tile), BF16),
            pltpu.VMEM((4, tokens, room), BF16),
            pltpu.VMEM((4, tokens, tile), F32),
            pltpu.VMEM((2, tokens, tile), F32),
            pltpu.VMEM((3, 2, tokens, tile), BF16),
            pltpu.VMEM((3, tiles, tokens, tile), BF16),
            pltpu.VMEM((2, tokens, tile), F32),
            pltpu.VMEM((2, tokens, tile), BF16),
            pltpu.SemaphoreType.DMA((experts,)),
            pltpu.SemaphoreType.DMA((4,)),
            pltpu.SemaphoreType.DMA((2,)),
            pltpu.SemaphoreType.DMA((2,)),
            pltpu.SemaphoreType.DMA((3, count)),
            pltpu.SemaphoreType.DMA((3, count)),
        ],
        compiler_params=pltpu.CompilerParams(vmem_limit_bytes=63 * 2**20, collective_id=0, has_side_effects=True),
        cost_estimate=pl.CostEstimate(
            flops=2 * experts * 4 * SEG * width * ff, bytes_accessed=experts * width * ff * 2, transcendentals=0
        ),
        name="down",
    )(table, h, wd, shared)


def solution(mesh):
    members = mesh.shape["ep"]

    def move(v, hop):
        return lax.ppermute(v, "ep", [(i, i ^ hop) for i in range(members)])

    def body(x, expert, slot, gate, wg, wu, wd, sg, su, sd):
        x, expert, slot, gate = (v[0, 0] for v in (x, expert, slot, gate))
        local = wg.shape[0]
        me = lax.axis_index("ep")

        hit = (expert.T[None] == jnp.arange(local * members)[:, None, None]) & (slot.T < SEG)[None]
        slots = jnp.max(jnp.where(hit, slot.T[None], -1), axis=1)
        gates = jnp.sum(jnp.where(hit, gate.T.astype(BF16).astype(F32)[None], 0.0), axis=1)
        table = jnp.stack([slots.astype(F32), gates])
        parts = []
        for hop in range(members):
            part = lax.dynamic_slice_in_dim(table, (me ^ hop) * local, local, axis=1)
            parts.append(move(part, hop) if hop else part)

        far = [move(x[:, :FIRST], 2)]
        near = move(x, 1)

        shared, rest_x = shared_call(x, sg, su, sd)
        far.append(move(rest_x, 2))

        shared, far[0] = lax.optimization_barrier((shared, far[0]))
        table = jnp.stack(parts)
        npad = (jnp.max(table[:, 0], axis=2).astype(jnp.int32) + 16) // 16 * 16
        sums = up_call(0, FIRST, npad, table, (x, near, far[0], move(far[0], 1)), wg, wu)
        sums, far[1] = lax.optimization_barrier((sums, far[1]))
        rest = x.shape[1] - FIRST
        h = up_call(FIRST, rest, npad, table, (x, near, far[1], move(far[1], 1)), wg, wu, sums)
        return down_call(table, h, wd, shared)[None, None]

    tok, exp, whole = P("dp", "ep", None, None), P("ep", None, None), P(None, None)

    return jax.shard_map(
        body,
        mesh=mesh,
        in_specs=(tok, tok, tok, tok, exp, exp, exp, whole, whole, whole),
        out_specs=tok,
        check_vma=False,
    )
```

```python
import functools

import jax
import jax.numpy as jnp
from jax import lax
from jax.experimental import pallas as pl
from jax.experimental.pallas import tpu as pltpu
from jax.sharding import PartitionSpec as P


FIRST = 3328
EARLY = 4
UNIT = 256
HALF = 160
SEG = 80
MESH = pl.DeviceIdType.MESH
F32, BF16 = jnp.float32, jnp.bfloat16
ANY = pl.BlockSpec(memory_space=pl.ANY)
VMEM = pl.BlockSpec(memory_space=pltpu.VMEM)
SMEM = pl.BlockSpec(memory_space=pltpu.SMEM)


def offsets(npad, e):
    offs, total = [], 0
    for k in range(4):
        offs.append(total)
        total = total + npad[k, e]
    return offs, total


def place(offs, k):
    return pl.ds(pl.multiple_of(offs[k], 16), SEG)


def dispatch(npad, table, e, xv, z):
    offs, _ = offsets(npad, e)
    line = lax.broadcasted_iota(jnp.int32, (SEG, table.shape[3]), 0).astype(F32)
    for k in range(4):
        pick = jnp.where(line == table[k, 0, pl.ds(e, 1), :], 1.0, 0.0).astype(BF16)
        z[place(offs, k), :] = jnp.dot(pick, xv[k], preferred_element_type=F32).astype(BF16)


def for_rows(total, work):
    for low, high in ((n, n + SEG) for n in range(0, 4 * SEG, SEG)):

        @pl.when((total > low) & (total <= high))
        def _():
            work(high)


def arrange(npad, experts, order):
    half = experts // 2
    totals = [offsets(npad, e)[1] for e in range(experts)]
    for e in range(experts):
        rank = jnp.int32(0)
        for o in range(experts):
            if o != e:
                ahead = totals[o] >= totals[e] if o < e else totals[o] > totals[e]
                rank = rank + ahead.astype(jnp.int32)
        order[jnp.where(rank < half, 2 * (half - 1 - rank), 2 * (rank - half) + 1)] = e


def sums_copies(npad, e, near, away, sem, act, out):
    _, total = offsets(npad, e)
    for b in range(4):
        band = pl.ds(b * SEG, SEG)

        @pl.when(total > b * SEG)
        def _():
            pair = near.at[:, band], away.at[:, band]
            act(pltpu.make_async_copy(*(pair if out else pair[::-1]), sem.at[b]))


def start(copy):
    copy.start()


def wait(copy):
    copy.wait()


def first_kernel(tile, depth, npad, table, x0, x1, x2, x3, wg, wu, sums, xv, z, wbuf, abuf, order, xsem, wsem, asem):
    experts, rows = sums.shape[0], z.shape[1]
    per = wg.shape[2] // tile
    steps = experts * per
    units = tile // UNIT

    def weights(i):
        e, cols, s = order[i // per], pl.ds(pl.multiple_of((i % per) * tile, tile), tile), i % depth
        return [
            pltpu.make_async_copy(
                w.at[e, pl.ds(0, rows), cols], wbuf.at[s, n], wsem.at[s, n]
            )
            for n, w in enumerate((wg, wu))
        ]

    def keep(i, act):
        e, s = order[i // per], i % 2
        sums_copies(npad, e, abuf.at[s], sums.at[i // per, pl.ds((i % per) * units, units)], asem.at[s], act, True)

    blocks = []
    for k, x in enumerate((x0, x1, x2, x3)):
        part = x if x.shape[1] == rows else x.at[:, pl.ds(0, rows)]
        blocks.append(pltpu.make_async_copy(part, xv.at[k], xsem.at[k]))
    for c in blocks:
        c.start()
    arrange(npad, wg.shape[0], order)
    for i in range(depth):
        for c in weights(i):
            c.start()
    for c in blocks:
        c.wait()

    def step(i, _):
        e, s = order[i // per], i % depth
        _, total = offsets(npad, e)

        @pl.when(i % per == 0)
        def _():
            dispatch(npad, table, e, xv, z)

        for c in weights(i):
            c.wait()

        @pl.when(i >= 2)
        def _():
            keep(i - 2, wait)

        def work(n):
            for m in range(2):
                half = jnp.dot(z[:n, :], wbuf[s, m], preferred_element_type=F32)
                for v in range(units):
                    abuf[i % 2, v, :n, m * UNIT : (m + 1) * UNIT] = half[:, v * UNIT : (v + 1) * UNIT]

        for_rows(total, work)

        @pl.when(i + depth < steps)
        def _():
            for c in weights(i + depth):
                c.start()

        keep(i, start)
        return 0

    lax.fori_loop(0, steps, step, 0)
    for i in (steps - 2, steps - 1):
        keep(jnp.int32(i), wait)


def rest_kernel(depth, npad, table, x0, x1, f0, d0, f1, d1, wg, wu, sums, h, xv, z, wbuf, abuf, hbuf, hout, order, xsem, wsem, asem, hsem):
    experts, rows, ff = wg.shape
    part = sums.shape[0]
    first = f0.shape[1]
    per = ff // UNIT
    begun, steps = part * per, experts * per

    def weights(i, low):
        e, cols, s = order[i // per], pl.ds(pl.multiple_of((i % per) * UNIT, UNIT), UNIT), i % depth
        band = pl.ds(low, rows - low)
        return [
            pltpu.make_async_copy(w.at[e, band, cols], wbuf.at[s, n, band], wsem.at[s, n])
            for n, w in enumerate((wg, wu))
        ]

    def resume(i, act):
        e, s = order[i // per], i % depth
        sums_copies(npad, e, abuf.at[pl.ds(s, 1)], sums.at[i // per, pl.ds(i % per, 1)], asem.at[s], act, False)

    def ask(i, low):
        for c in weights(i, low):
            c.start()
        if low:
            resume(i, start)

    def result(n):
        return pltpu.make_async_copy(hout.at[n % 2], h.at[order[n]], hsem.at[n % 2])

    blocks = [pltpu.make_async_copy(x, xv.at[k], xsem.at[k]) for k, x in enumerate((x0, x1))]
    for n, (a, b) in enumerate(((f0, f1), (d0, d1))):
        blocks.append(pltpu.make_async_copy(a, xv.at[2 + n, :, pl.ds(0, first)], xsem.at[2 + 2 * n]))
        blocks.append(pltpu.make_async_copy(b, xv.at[2 + n, :, pl.ds(first, rows - first)], xsem.at[3 + 2 * n]))
    for c in blocks:
        c.start()
    arrange(npad, experts, order)
    for i in range(depth):
        ask(i, first)
    for c in blocks:
        c.wait()

    def step(low, i):
        n, j, s = i // per, i % per, i % depth
        e = order[n]
        offs, total = offsets(npad, e)

        @pl.when(j == 0)
        def _():
            dispatch(npad, table, e, xv.at[:, :, low:], z.at[:, low:])

        for c in weights(i, low):
            c.wait()
        if low:
            resume(i, wait)

        def work(n):
            g, u = (jnp.dot(z[:n, low:], wbuf[s, m, low:], preferred_element_type=F32) for m in range(2))
            if low:
                g, u = g + abuf[s, :n, :UNIT], u + abuf[s, :n, UNIT:]
            hbuf[:n, pl.ds(pl.multiple_of(j * UNIT, UNIT), UNIT)] = (jax.nn.silu(g) * u).astype(BF16)

        for_rows(total, work)

        if low:

            @pl.when(i + depth < begun)
            def _():
                ask(i + depth, low)

            @pl.when(i + depth >= begun)
            def _():
                ask(i + depth, 0)
        else:

            @pl.when(i + depth < steps)
            def _():
                ask(i + depth, 0)

        @pl.when(j == per - 1)
        def _():
            @pl.when(n >= 2)
            def _():
                result(n - 2).wait()

            line = lax.broadcasted_iota(jnp.int32, (SEG, ff), 0)
            for k in range(4):
                band = hbuf[place(offs, k), :]
                hout[n % 2, SEG * k : SEG * (k + 1), :] = jnp.where(line < npad[k, e], band, jnp.zeros_like(band))
            result(n).start()

        return 0

    lax.fori_loop(0, begun, lambda i, _: step(first, i), 0)
    lax.fori_loop(begun, steps, lambda i, _: step(0, i), 0)
    for n in (experts - 2, experts - 1):
        result(n).wait()


def expert_params(experts, rows, ff):
    return dict(
        compiler_params=pltpu.CompilerParams(vmem_limit_bytes=63 * 2**20),
        cost_estimate=pl.CostEstimate(
            flops=4 * experts * HALF * rows * ff, bytes_accessed=experts * rows * ff * 4, transcendentals=0
        ),
    )


def first_call(experts, npad, table, xs, wg, wu):
    ff, (tokens, rows) = wg.shape[2], xs[2].shape
    tile, depth = 512, 3
    return pl.pallas_call(
        functools.partial(first_kernel, tile, depth),
        out_shape=jax.ShapeDtypeStruct((experts, ff // UNIT, 2 * HALF, 2 * UNIT), F32),
        in_specs=[SMEM, VMEM] + [ANY] * 6,
        out_specs=ANY,
        scratch_shapes=[
            pltpu.VMEM((4, tokens, rows), BF16),
            pltpu.VMEM((2 * HALF, rows), BF16),
            pltpu.VMEM((depth, 2, rows, tile), BF16),
            pltpu.VMEM((2, tile // UNIT, 2 * HALF, 2 * UNIT), F32),
            pltpu.SMEM((wg.shape[0],), jnp.int32),
            pltpu.SemaphoreType.DMA((4,)),
            pltpu.SemaphoreType.DMA((depth, 2)),
            pltpu.SemaphoreType.DMA((2, 4)),
        ],
        name="up_first",
        **expert_params(experts, rows, ff),
    )(npad, table, *xs, wg, wu)


def rest_call(npad, table, xs, wg, wu, sums):
    (experts, rows, ff), tokens, depth = wg.shape, xs[0].shape[0], 4
    return pl.pallas_call(
        functools.partial(rest_kernel, depth),
        out_shape=jax.ShapeDtypeStruct((experts, 2 * HALF, ff), BF16),
        in_specs=[SMEM, VMEM] + [ANY] * 9,
        out_specs=ANY,
        scratch_shapes=[
            pltpu.VMEM((4, tokens, rows), BF16),
            pltpu.VMEM((2 * HALF, rows), BF16),
            pltpu.VMEM((depth, 2, rows, UNIT), BF16),
            pltpu.VMEM((depth, 2 * HALF, 2 * UNIT), F32),
            pltpu.VMEM((2 * HALF, ff), BF16),
            pltpu.VMEM((2, 2 * HALF, ff), BF16),
            pltpu.SMEM((experts,), jnp.int32),
            pltpu.SemaphoreType.DMA((6,)),
            pltpu.SemaphoreType.DMA((depth, 2)),
            pltpu.SemaphoreType.DMA((depth, 4)),
            pltpu.SemaphoreType.DMA((2,)),
        ],
        name="up_rest",
        **expert_params(experts, rows, ff),
    )(npad, table, *xs, wg, wu, sums)


def shared_kernel(tile, wide, depth, x, sg, su, sd, y, rest, xv, wbuf, dbuf, hbuf, ybuf, xsem, wsem, dsem, ysem):
    ff, width = sd.shape
    ups, downs = ff // tile, width // wide

    def block(n, size):
        return pl.ds(pl.multiple_of(n * size, size), size)

    def up(i):
        return [
            pltpu.make_async_copy(
                w.at[:, block(i, tile)], wbuf.at[i % depth, :, pl.ds(n * tile, tile)], wsem.at[i % depth, n]
            )
            for n, w in enumerate((sg, su))
        ]

    def down(t):
        return pltpu.make_async_copy(sd.at[:, block(t, wide)], dbuf.at[t % depth], dsem.at[t % depth])

    def result(t):
        return pltpu.make_async_copy(ybuf.at[t % 2], y.at[:, block(t, wide)], ysem.at[t % 2])

    load = pltpu.make_async_copy(x, xv, xsem)
    load.start()
    for i in range(depth):
        for c in up(i):
            c.start()
    load.wait()
    split = pltpu.make_async_copy(xv.at[:, x.shape[1] - rest.shape[1] :], rest, xsem)
    split.start()

    def raise_(i, _):
        for c in up(i):
            c.wait()
        gu = jnp.dot(xv[...], wbuf[i % depth], preferred_element_type=F32)
        hbuf[:, block(i, tile)] = (jax.nn.silu(gu[:, :tile]) * gu[:, tile:]).astype(BF16)

        @pl.when(i + depth < ups)
        def _():
            for c in up(i + depth):
                c.start()

        @pl.when(i >= ups - depth)
        def _():
            down(i - (ups - depth)).start()

        return 0

    lax.fori_loop(0, ups, raise_, 0)

    def lower(t, _):
        down(t).wait()

        @pl.when(t >= 2)
        def _():
            result(t - 2).wait()

        ybuf[t % 2] = jnp.dot(hbuf[...], dbuf[t % depth], preferred_element_type=F32)
        result(t).start()

        @pl.when(t + depth < downs)
        def _():
            down(t + depth).start()

        return 0

    lax.fori_loop(0, downs, lower, 0)
    for t in (downs - 2, downs - 1):
        result(t).wait()
    split.wait()


def shared_call(x, sg, su, sd):
    tokens, rows = x.shape
    ff, width = sd.shape
    tile, wide, depth = 256, 1024, 4
    return pl.pallas_call(
        functools.partial(shared_kernel, tile, wide, depth),
        out_shape=[
            jax.ShapeDtypeStruct((tokens, width), F32),
            jax.ShapeDtypeStruct((tokens, rows - FIRST), BF16),
        ],
        in_specs=[ANY] * 4,
        out_specs=[ANY] * 2,
        scratch_shapes=[
            pltpu.VMEM((tokens, rows), BF16),
            pltpu.VMEM((depth, rows, 2 * tile), BF16),
            pltpu.VMEM((depth, ff, wide), BF16),
            pltpu.VMEM((tokens, ff), BF16),
            pltpu.VMEM((2, tokens, wide), F32),
            pltpu.SemaphoreType.DMA,
            pltpu.SemaphoreType.DMA((depth, 2)),
            pltpu.SemaphoreType.DMA((depth,)),
            pltpu.SemaphoreType.DMA((2,)),
        ],
        compiler_params=pltpu.CompilerParams(vmem_limit_bytes=63 * 2**20),
        cost_estimate=pl.CostEstimate(
            flops=6 * tokens * rows * ff, bytes_accessed=6 * rows * ff, transcendentals=0
        ),
        name="shared",
    )(x, sg, su, sd)


def down_kernel(tile, small, table, h, wd, shared, y, hv, wbuf, rows, mix, own, far32, outs, lands, sbuf, ybuf, hsem, wsem, ssem, ysem, send, recv):
    experts, _, width = wd.shape
    _, room = mix.shape[1:]
    pairs = experts // 2
    many = width // tile - 1
    few = tile // small
    me = lax.axis_index("ep")
    near, far = me + 1 - 2 * (me % 2), (me + 2) % 4

    barrier = pltpu.get_barrier_semaphore()
    for d in (near, far):
        pl.semaphore_signal(barrier, inc=1, device_id={"ep": d}, device_id_type=MESH)

    class Tile:
        def __init__(self, t, part=None):
            self.t = t if part is None else many + part
            self.n = tile if part is None else small
            start = t * tile if part is None else many * tile + part * small
            self.columns = pl.ds(pl.multiple_of(start, small), self.n)
            self.place = t if part is None else many
            self.inside = pl.ds(0 if part is None else part * small, self.n)

        def addend(self):
            s = self.t % 2
            return pltpu.make_async_copy(shared.at[:, self.columns], sbuf.at[s, :, : self.n], ssem.at[s])

        def result(self):
            s = self.t % 2
            return pltpu.make_async_copy(ybuf.at[s, :, : self.n], y.at[:, self.columns], ysem.at[s])

        def sending(self, kind):
            return pltpu.make_async_remote_copy(
                src_ref=outs.at[kind, self.t % 2, :, : self.n],
                dst_ref=lands.at[kind, self.place, :, self.inside],
                send_sem=send.at[kind, self.t],
                recv_sem=recv.at[kind, self.t],
                device_id={"ep": far if kind == 2 else near},
                device_id_type=MESH,
            )

        def combine(self, older):
            n, s = self.n, self.t % 2

            def free(old):
                old.sending(0).wait_send()
                old.sending(1).wait_send()

            older(free)
            outs[0, s, :, :n] = jnp.dot(mix[1], rows[1, :, :n], preferred_element_type=F32).astype(BF16)
            outs[1, s, :, :n] = jnp.dot(mix[3], rows[3, :, :n], preferred_element_type=F32).astype(BF16)
            far32[s, :, :n] = jnp.dot(mix[2], rows[2, :, :n], preferred_element_type=F32)
            own[self.t % 4, :, :n] = jnp.dot(mix[0], rows[0, :, :n], preferred_element_type=F32)
            self.sending(1).start()
            self.sending(0).start()

        def forward(self, older):
            n, s = self.n, self.t % 2
            self.sending(1).wait_recv()
            older(lambda old: old.sending(2).wait_send())
            outs[2, s, :, :n] = (far32[s, :, :n] + lands[1, self.place, :, self.inside].astype(F32)).astype(BF16)
            self.sending(2).start()

        def final(self, older, newer):
            n, s = self.n, self.t % 2
            self.sending(0).wait_recv()
            self.sending(2).wait_recv()
            self.addend().wait()
            older(lambda old: old.result().wait())
            local = own[self.t % 4, :, :n] + sbuf[s, :, :n]
            rest = (lands[k, self.place, :, self.inside].astype(F32) for k in (0, 2))
            ybuf[s, :, :n] = (local + next(rest) + next(rest)).astype(BF16)
            self.result().start()
            newer(lambda new: new.addend().start())

    def weights(t, p):
        q = (t.t * pairs + p) % 2
        return [
            pltpu.make_async_copy(
                wd.at[2 * p + m, :, t.columns], wbuf.at[2 * q + m, :, : t.n], wsem.at[2 * q + m]
            )
            for m in range(2)
        ]

    def start(copies):
        for c in copies:
            c.start()

    def load(e):
        return pltpu.make_async_copy(h.at[e], hv.at[e], hsem.at[e])

    def multiply(t, p):
        q = (t.t * pairs + p) % 2
        for c in weights(t, p):
            c.wait()
        for m in range(2):
            e = 2 * p + m
            o = jnp.dot(hv[e], wbuf[2 * q + m, :, : t.n], preferred_element_type=F32).astype(BF16)
            for k in range(4):
                rows[k, pl.ds(pl.multiple_of(e * SEG, 16), SEG), : t.n] = o[SEG * k : SEG * (k + 1)]

    for p in range(2):
        load(2 * p).start()
        load(2 * p + 1).start()
        start(weights(Tile(0), p))
    for e in range(4, experts):
        load(e).start()
    for t in range(2):
        Tile(t).addend().start()

    place, row = (lax.broadcasted_iota(jnp.int32, (experts, room), d) for d in (1, 0))
    spread = jnp.where((place >= SEG * row) & (place < SEG * (row + 1)), 1.0, 0.0).astype(BF16)
    place = lax.broadcasted_iota(jnp.int32, (1, room), 1)
    slot = place
    for e in range(1, experts):
        slot = jnp.where(place >= SEG * e, place - SEG * e, slot)
    slot = slot.astype(F32)
    for k in range(4):
        s, g = (
            lax.dot_general(table[k, n].astype(BF16), spread, (((0,), (0,)), ((), ())), preferred_element_type=F32)
            for n in range(2)
        )
        mix[k] = jnp.where(s == slot, g, 0.0).astype(BF16)
    pl.semaphore_wait(barrier, 2)

    def step(i, _):
        t, p = i // pairs, i % pairs
        this = Tile(t)

        def back(least, distance):
            def older(act):
                @pl.when(t >= least)
                def _():
                    act(Tile(t - distance))

            return older

        @pl.when(t == 0)
        def _():
            load(2 * p).wait()
            load(2 * p + 1).wait()

        multiply(this, p)

        @pl.when(i + 2 < many * pairs)
        def _():
            start(weights(Tile((i + 2) // pairs), (i + 2) % pairs))

        @pl.when(i + 2 >= many * pairs)
        def _():
            start(weights(Tile(0, 0), i + 2 - many * pairs))

        @pl.when((p == 0) & (t >= 1))
        def _():
            Tile(t - 1).forward(back(3, 3))

        @pl.when((p == 2) & (t >= 2))
        def _():
            Tile(t - 2).final(back(4, 4), lambda act: act(Tile(t)))

        @pl.when(p == pairs - 1)
        def _():
            this.combine(back(2, 2))

        return 0

    lax.fori_loop(0, many * pairs, step, 0)

    tiles = [Tile(t) for t in range(many)] + [Tile(0, m) for m in range(few)]

    def at(n):
        return lambda act: act(tiles[n])

    for n in range(many, many + few):

        def step2(p, _):
            multiply(tiles[n], p)

            @pl.when(p + 2 < pairs)
            def _():
                start(weights(tiles[n], p + 2))

            if n + 1 < many + few:

                @pl.when(p + 2 >= pairs)
                def _():
                    start(weights(tiles[n + 1], p + 2 - pairs))

            @pl.when(p == 0)
            def _():
                tiles[n - 1].forward(at(n - 3))

            @pl.when(p == 2)
            def _():
                tiles[n - 2].final(at(n - 4), at(n))

            return 0

        lax.fori_loop(0, pairs, step2, 0)
        tiles[n].combine(at(n - 2))
    last = many + few - 1
    tiles[last].forward(at(last - 2))
    tiles[last - 1].final(at(last - 3), lambda act: None)
    tiles[last].final(at(last - 2), lambda act: None)
    for t in tiles[-2:]:
        t.result().wait()
        for kind in range(3):
            t.sending(kind).wait_send()


def down_call(table, h, wd, shared):
    experts, ff, width = wd.shape
    tile, small = 1024, 512
    tiles = width // tile
    count = tiles - 1 + tile // small
    tokens = table.shape[3]
    room = SEG * experts
    return pl.pallas_call(
        functools.partial(down_kernel, tile, small),
        out_shape=jax.ShapeDtypeStruct((tokens, width), BF16),
        in_specs=[VMEM, ANY, ANY, ANY],
        out_specs=ANY,
        scratch_shapes=[
            pltpu.VMEM((experts, 4 * SEG, ff), BF16),
            pltpu.VMEM((4, ff, tile), BF16),
            pltpu.VMEM((4, room, tile), BF16),
            pltpu.VMEM((4, tokens, room), BF16),
            pltpu.VMEM((4, tokens, tile), F32),
            pltpu.VMEM((2, tokens, tile), F32),
            pltpu.VMEM((3, 2, tokens, tile), BF16),
            pltpu.VMEM((3, tiles, tokens, tile), BF16),
            pltpu.VMEM((2, tokens, tile), F32),
            pltpu.VMEM((2, tokens, tile), BF16),
            pltpu.SemaphoreType.DMA((experts,)),
            pltpu.SemaphoreType.DMA((4,)),
            pltpu.SemaphoreType.DMA((2,)),
            pltpu.SemaphoreType.DMA((2,)),
            pltpu.SemaphoreType.DMA((3, count)),
            pltpu.SemaphoreType.DMA((3, count)),
        ],
        compiler_params=pltpu.CompilerParams(vmem_limit_bytes=63 * 2**20, collective_id=0, has_side_effects=True),
        cost_estimate=pl.CostEstimate(
            flops=2 * experts * 4 * SEG * width * ff, bytes_accessed=experts * width * ff * 2, transcendentals=0
        ),
        name="down",
    )(table, h, wd, shared)


def solution(mesh):
    members = mesh.shape["ep"]

    def move(v, hop):
        return lax.ppermute(v, "ep", [(i, i ^ hop) for i in range(members)])

    def body(x, expert, slot, gate, wg, wu, wd, sg, su, sd):
        x, expert, slot, gate = (v[0, 0] for v in (x, expert, slot, gate))
        local = wg.shape[0]
        me = lax.axis_index("ep")

        hit = (expert.T[None] == jnp.arange(local * members)[:, None, None]) & (slot.T < SEG)[None]
        slots = jnp.max(jnp.where(hit, slot.T[None], -1), axis=1)
        gates = jnp.sum(jnp.where(hit, gate.T.astype(BF16).astype(F32)[None], 0.0), axis=1)
        table = jnp.stack([slots.astype(F32), gates])
        parts = []
        for hop in range(members):
            part = lax.dynamic_slice_in_dim(table, (me ^ hop) * local, local, axis=1)
            parts.append(move(part, hop) if hop else part)

        far = [move(x[:, :FIRST], 2)]
        near = move(x, 1)

        shared, rest_x = shared_call(x, sg, su, sd)
        far.append(move(rest_x, 2))

        shared, far[0] = lax.optimization_barrier((shared, far[0]))
        table = jnp.stack(parts)
        npad = (jnp.max(table[:, 0], axis=2).astype(jnp.int32) + 16) // 16 * 16
        diag = [move(far[0], 1)]
        sums = first_call(EARLY, npad, table, (x, near, far[0], diag[0]), wg, wu)
        sums, far[1] = lax.optimization_barrier((sums, far[1]))
        diag.append(move(far[1], 1))
        h = rest_call(npad, table, (x, near, far[0], diag[0], far[1], diag[1]), wg, wu, sums)
        return down_call(table, h, wd, shared)[None, None]

    tok, exp, whole = P("dp", "ep", None, None), P("ep", None, None), P(None, None)

    return jax.shard_map(
        body,
        mesh=mesh,
        in_specs=(tok, tok, tok, tok, exp, exp, exp, whole, whole, whole),
        out_specs=tok,
        check_vma=False,
    )
```
